32 devices in a mesh: dp: 2 (over x), tp: 4 (over z), cp: 4 (over y, core).
Axes of the slice: x: 2, y: 2, z: 4, core: 2. Of those that a mesh axis runs over, the one named last changes fastest.
Arguments:
- hidden: bfloat16 [6, 1536, 5120], P('dp', 'cp'), parts along dimension 0
- positions: int32 [6, 1536], P('dp', 'cp'), parts along dimension 0
- w_dq: bfloat16 [5120, 1536], replicated
- g_q: float32 [1536], replicated
- w_uq: bfloat16 [1536, 24576], P(None, 'tp')
- w_dkv: bfloat16 [5120, 576], replicated
- g_kv: float32 [512], replicated
- w_uk: bfloat16 [512, 16384], P(None, 'tp')
- w_uv: bfloat16 [512, 16384], P(None, 'tp')
- w_o: bfloat16 [16384, 5120], P('tp')
Outputs:
- output 1: bfloat16 [6, 1536, 5120], P('dp', 'cp'), parts along dimension 0
- output 2: bfloat16 [6, 1536, 512], P('dp', 'cp'), parts along dimension 0
- output 3: bfloat16 [6, 1536, 64], P('dp', 'cp'), parts along dimension 0
There are 2 independent parts. The reference program is written for one: setup_inputs(seed, part) draws one part's arguments, and reference() takes and returns one part's arrays. A program takes and returns all parts, laid end to end along the dimension named above; an argument that names none is the same for every part.
All inputs are finite; a program needn't handle non-finite values.
Results may differ from the reference program's by a relative error of at most 0.0075555.
Values are sent between devices in bfloat16 or wider.
A program may use at most 1 GiB of HBM per device.

```python
import jax
import jax.numpy as jnp
from jax import lax

N_SEQ = 3
SEQ_LEN = 1536
CP_SIZE = 4
D_MODEL = 5120
N_HEADS = 128
Q_RANK = 1536
KV_RANK = 512
NOPE_DIM = 128
ROPE_DIM = 64
V_DIM = 128

QK_DIM = NOPE_DIM + ROPE_DIM
BLOCK_LEN = SEQ_LEN // (2 * CP_SIZE)
SOFT_SCALE = QK_DIM ** -0.5
ROPE_BASE = 10000.0
NORM_EPS = 1e-6
Q_GAIN = 3.0


def draw_positions(rng_key):
    base_ids = jnp.tile(jnp.arange(CP_SIZE, dtype=jnp.int32)[None, :], (N_SEQ, 1))
    pair_ids = jax.random.permutation(rng_key, base_ids, axis=1, independent=True)
    offsets = jnp.arange(BLOCK_LEN, dtype=jnp.int32)
    first_blocks = pair_ids[:, :, None] * BLOCK_LEN + offsets
    second_blocks = (2 * CP_SIZE - 1 - pair_ids)[:, :, None] * BLOCK_LEN + offsets
    return jnp.stack([first_blocks, second_blocks], axis=2).reshape(N_SEQ, SEQ_LEN)


def draw_normal(rng_key, tensor_shape, std_dev):
    return (jax.random.normal(rng_key, tensor_shape, jnp.float32) * std_dev).astype(jnp.bfloat16)


def setup_inputs(seed: int = 0, part: int = 0) -> dict:
    root_key = jax.random.key(seed)
    part_key = jax.random.fold_in(root_key, part)
    weight_keys = jax.random.split(jax.random.key(seed + 1), 8)
    hidden = draw_normal(jax.random.fold_in(part_key, 0), (N_SEQ, SEQ_LEN, D_MODEL), 1.0)
    positions = draw_positions(jax.random.fold_in(part_key, 1))
    w_dq = draw_normal(weight_keys[0], (D_MODEL, Q_RANK), D_MODEL ** -0.5)
    g_q = jax.random.uniform(weight_keys[1], (Q_RANK,), jnp.float32, 0.5, 1.5)
    w_uq = draw_normal(weight_keys[2], (Q_RANK, N_HEADS * QK_DIM), Q_GAIN * Q_RANK ** -0.5)
    w_dkv = draw_normal(weight_keys[3], (D_MODEL, KV_RANK + ROPE_DIM), D_MODEL ** -0.5)
    g_kv = jax.random.uniform(weight_keys[4], (KV_RANK,), jnp.float32, 0.5, 1.5)
    w_uk = draw_normal(weight_keys[5], (KV_RANK, N_HEADS * NOPE_DIM), KV_RANK ** -0.5)
    w_uv = draw_normal(weight_keys[6], (KV_RANK, N_HEADS * V_DIM), KV_RANK ** -0.5)
    w_o = draw_normal(weight_keys[7], (N_HEADS * V_DIM, D_MODEL), (N_HEADS * V_DIM) ** -0.5)
    return {'hidden': hidden, 'positions': positions, 'w_dq': w_dq, 'g_q': g_q, 'w_uq': w_uq,
            'w_dkv': w_dkv, 'g_kv': g_kv, 'w_uk': w_uk, 'w_uv': w_uv, 'w_o': w_o}


def rms_norm(tensor, norm_gain):
    tensor_f32 = tensor.astype(jnp.float32)
    inv_rms = lax.rsqrt(jnp.mean(tensor_f32 * tensor_f32, axis=-1, keepdims=True) + NORM_EPS)
    return (tensor_f32 * inv_rms * norm_gain).astype(jnp.bfloat16)


def rotate(tensor, cos_t, sin_t):
    tensor_f32 = tensor.astype(jnp.float32)
    half_dim = tensor_f32.shape[-1] // 2
    lower_half = tensor_f32[..., :half_dim]
    upper_half = tensor_f32[..., half_dim:]
    return jnp.concatenate([lower_half * cos_t - upper_half * sin_t,
                            lower_half * sin_t + upper_half * cos_t], axis=-1).astype(jnp.bfloat16)


def reference(hidden, positions, w_dq, g_q, w_uq, w_dkv, g_kv, w_uk, w_uv, w_o):
    inv_freq = ROPE_BASE ** (-2.0 * jnp.arange(ROPE_DIM // 2, dtype=jnp.float32) / ROPE_DIM)

    def one_sequence(seq_args):
        x_seq, pos_seq = seq_args
        angles = pos_seq.astype(jnp.float32)[:, None] * inv_freq[None, :]
        cos_t = jnp.cos(angles)
        sin_t = jnp.sin(angles)
        q_latent = jnp.dot(x_seq, w_dq, preferred_element_type=jnp.float32).astype(jnp.bfloat16)
        q_normed = rms_norm(q_latent, g_q)
        q_full = jnp.dot(q_normed, w_uq, preferred_element_type=jnp.float32).astype(jnp.bfloat16)
        q_full = q_full.reshape(SEQ_LEN, N_HEADS, QK_DIM)
        q_nope = q_full[:, :, :NOPE_DIM]
        q_rope = rotate(q_full[:, :, NOPE_DIM:], cos_t[:, None, :], sin_t[:, None, :])
        kv_joint = jnp.dot(x_seq, w_dkv, preferred_element_type=jnp.float32).astype(jnp.bfloat16)
        latent = rms_norm(kv_joint[:, :KV_RANK], g_kv)
        k_rope = rotate(kv_joint[:, KV_RANK:], cos_t, sin_t)
        k_nope = jnp.dot(latent, w_uk, preferred_element_type=jnp.float32).astype(jnp.bfloat16)
        k_nope = k_nope.reshape(SEQ_LEN, N_HEADS, NOPE_DIM)
        values = jnp.dot(latent, w_uv, preferred_element_type=jnp.float32).astype(jnp.bfloat16)
        values = values.reshape(SEQ_LEN, N_HEADS, V_DIM)
        allowed = pos_seq[None, :] <= pos_seq[:, None]

        def one_head(head_args):
            qn_head, qr_head, kn_head, v_head = head_args
            scores = (jnp.dot(qn_head, kn_head.T, preferred_element_type=jnp.float32)
                      + jnp.dot(qr_head, k_rope.T, preferred_element_type=jnp.float32)) * SOFT_SCALE
            scores = jnp.where(allowed, scores, -jnp.inf)
            probs_bf = jax.nn.softmax(scores, axis=-1).astype(jnp.bfloat16)
            return jnp.dot(probs_bf, v_head, preferred_element_type=jnp.float32).astype(jnp.bfloat16)

        heads_out = lax.map(one_head, (jnp.swapaxes(q_nope, 0, 1), jnp.swapaxes(q_rope, 0, 1),
                                       jnp.swapaxes(k_nope, 0, 1), jnp.swapaxes(values, 0, 1)))
        attn_out = jnp.swapaxes(heads_out, 0, 1).reshape(SEQ_LEN, N_HEADS * V_DIM)
        y_seq = (x_seq.astype(jnp.float32)
                 + jnp.dot(attn_out, w_o, preferred_element_type=jnp.float32)).astype(jnp.bfloat16)
        return y_seq, latent, k_rope

    out_hidden, latent, k_rope = lax.map(one_sequence, (hidden, positions))
    return out_hidden, latent, k_rope
```

```python
import functools

import jax
import jax.numpy as jnp
from jax import lax
from jax.experimental import pallas as pl
from jax.experimental.pallas import tpu as pltpu
from jax.sharding import PartitionSpec as P


ROPE_BASE = 10000.0
NORM_EPS = 1e-6
LOG2_E = 1.4426950408889634
CHUNKS = 24
PAIR = 2
SPLITS = 3


def rms_norm(tensor, norm_gain):
    tensor_f32 = tensor.astype(jnp.float32)
    inv_rms = lax.rsqrt(jnp.mean(tensor_f32 * tensor_f32, axis=-1, keepdims=True) + NORM_EPS)
    return (tensor_f32 * inv_rms * norm_gain).astype(jnp.bfloat16)


def rope_tables(positions, rope_dim):
    inv_freq = ROPE_BASE ** (-2.0 * jnp.arange(rope_dim // 2, dtype=jnp.float32) / rope_dim)
    angles = positions.astype(jnp.float32)[..., None] * inv_freq
    return jnp.cos(angles), jnp.sin(angles)


def rotate(tensor, cos_t, sin_t):
    tensor_f32 = tensor.astype(jnp.float32)
    half_dim = tensor_f32.shape[-1] // 2
    lower_half = tensor_f32[..., :half_dim]
    upper_half = tensor_f32[..., half_dim:]
    return jnp.concatenate([lower_half * cos_t - upper_half * sin_t,
                            lower_half * sin_t + upper_half * cos_t], axis=-1).astype(jnp.bfloat16)


def attend_kernel(soft_scale, order_ref, q_ref, cos_ref, sin_ref, lat_hbm, w_uk_ref, w_uv_ref, *rest):
    o_ref, lat_s, sems = rest[-3:]
    n_blocks, block_len, _ = lat_hbm.shape
    half_keys = n_blocks // 2 * block_len
    rank = w_uk_ref.shape[0]
    rope_dim = cos_ref.shape[1]
    nope_dim = w_uk_ref.shape[1] // PAIR
    v_dim = w_uv_ref.shape[1] // PAIR
    qk_dim = nope_dim + rope_dim

    @pl.when(pl.program_id(0) == 0)
    def _():
        copies = [pltpu.make_async_copy(lat_hbm.at[order_ref[j]], lat_s.at[pl.ds(j * block_len, block_len)], sems.at[j])
                  for j in range(n_blocks)]
        for copy in copies:
            copy.start()
        for copy in copies:
            copy.wait()

    low_id = order_ref[n_blocks]
    latent = lat_s[:, :rank]
    k_rope = lat_s[:, rank:rank + rope_dim]
    k_pair = jnp.dot(latent, w_uk_ref[...], preferred_element_type=jnp.float32).astype(jnp.bfloat16)
    v_pair = jnp.dot(latent, w_uv_ref[...], preferred_element_type=jnp.float32).astype(jnp.bfloat16)

    q_pair = q_ref[...].astype(jnp.float32)
    cos2 = cos_ref[...]
    sin2 = sin_ref[...]
    col_minus_row = (lax.broadcasted_iota(jnp.int32, (block_len, half_keys), 1)
                     - lax.broadcasted_iota(jnp.int32, (block_len, half_keys), 0))
    low_mask = col_minus_row <= low_id * block_len
    high_mask = col_minus_row <= (n_blocks - 1 - low_id) * block_len - half_keys
    factor = soft_scale * LOG2_E
    contract_last = (((1,), (1,)), ((), ()))

    for head in range(PAIR):
        q_head = q_pair if head == 0 else pltpu.roll(q_pair, (PAIR - head) * qk_dim, 1)
        q_rope = q_head[:, nope_dim:qk_dim]
        swapped = jnp.concatenate([q_rope[:, rope_dim // 2:], q_rope[:, :rope_dim // 2]], axis=1)
        q_rot = q_rope * cos2 + swapped * sin2
        q_cat = jnp.concatenate([q_head[:, :nope_dim], q_rot], axis=1).astype(jnp.bfloat16)
        k_cat = jnp.concatenate([k_pair[:, head * nope_dim:(head + 1) * nope_dim], k_rope], axis=1)
        v_head = v_pair[:, head * v_dim:(head + 1) * v_dim]
        early = lax.dot_general(q_cat, k_cat[:half_keys], contract_last, preferred_element_type=jnp.float32)
        late = lax.dot_general(q_cat[block_len:], k_cat[half_keys:], contract_last,
                               preferred_element_type=jnp.float32)

        low = jnp.where(low_mask, early[:block_len], -jnp.inf)
        low_exp = jnp.exp2((low - jnp.max(low, axis=1, keepdims=True)) * factor)
        low_prob = (low_exp * (1.0 / jnp.sum(low_exp, axis=1, keepdims=True))).astype(jnp.bfloat16)
        low_out = jnp.dot(low_prob, v_head[:half_keys], preferred_element_type=jnp.float32)

        near = early[block_len:]
        far = jnp.where(high_mask, late, -jnp.inf)
        top = jnp.maximum(jnp.max(near, axis=1, keepdims=True), jnp.max(far, axis=1, keepdims=True))
        near_exp = jnp.exp2((near - top) * factor)
        far_exp = jnp.exp2((far - top) * factor)
        inv_sum = 1.0 / (jnp.sum(near_exp, axis=1, keepdims=True) + jnp.sum(far_exp, axis=1, keepdims=True))
        high_out = (jnp.dot((near_exp * inv_sum).astype(jnp.bfloat16), v_head[:half_keys],
                            preferred_element_type=jnp.float32)
                    + jnp.dot((far_exp * inv_sum).astype(jnp.bfloat16), v_head[half_keys:],
                              preferred_element_type=jnp.float32))
        o_ref[:block_len, head * v_dim:(head + 1) * v_dim] = low_out.astype(jnp.bfloat16)
        o_ref[block_len:, head * v_dim:(head + 1) * v_dim] = high_out.astype(jnp.bfloat16)


def attend(q_full, cos2, sin2, lat_blocks, order, w_uk, w_uv, heads, soft_scale, pairs, prior):
    n_blocks, block_len, width = lat_blocks.shape
    tokens = q_full.shape[0]
    rank = w_uk.shape[0]
    keys = n_blocks * block_len
    qk_dim = q_full.shape[1] // heads
    nope_dim = w_uk.shape[1] // heads
    v_dim = w_uv.shape[1] // heads
    rope_dim = cos2.shape[1]
    first, count = pairs[0], len(pairs)
    flops = (2 * keys * rank * (nope_dim + v_dim) + 2 * tokens * keys * 3 // 4 * (qk_dim + v_dim)) * count * PAIR
    moved = 2 * (lat_blocks.size + (tokens * (qk_dim + v_dim) + rank * (nope_dim + v_dim)) * count * PAIR)
    in_specs = [
        pl.BlockSpec((tokens, PAIR * qk_dim), lambda h, order: (0, h + first)),
        pl.BlockSpec((tokens, rope_dim), lambda h, order: (0, 0)),
        pl.BlockSpec((tokens, rope_dim), lambda h, order: (0, 0)),
        pl.BlockSpec(memory_space=pl.ANY),
        pl.BlockSpec((rank, PAIR * nope_dim), lambda h, order: (0, h + first)),
        pl.BlockSpec((rank, PAIR * v_dim), lambda h, order: (0, h + first)),
    ]
    operands = [q_full, cos2, sin2, lat_blocks, w_uk, w_uv]
    aliases = {}
    if prior is not None:
        in_specs.append(pl.BlockSpec(memory_space=pl.ANY))
        operands.append(prior)
        aliases = {len(operands): 0}
    return pl.pallas_call(
        functools.partial(attend_kernel, soft_scale),
        out_shape=jax.ShapeDtypeStruct((tokens, heads * v_dim), jnp.bfloat16),
        grid_spec=pltpu.PrefetchScalarGridSpec(
            num_scalar_prefetch=1,
            grid=(count,),
            in_specs=in_specs,
            out_specs=pl.BlockSpec((tokens, PAIR * v_dim), lambda h, order: (0, h + first)),
            scratch_shapes=[pltpu.VMEM((keys, width), jnp.bfloat16), pltpu.SemaphoreType.DMA((n_blocks,))],
        ),
        input_output_aliases=aliases,
        compiler_params=pltpu.CompilerParams(dimension_semantics=("arbitrary",), vmem_limit_bytes=56 * 1024 * 1024),
        cost_estimate=pl.CostEstimate(flops=flops, bytes_accessed=moved,
                                      transcendentals=tokens * keys * count * PAIR * 3 // 4),
        name="attend",
    )(order, *operands)


def together(*values):
    return lax.optimization_barrier(values)


def chain_sum(partials, pieces, x_rows, n_tp, chunks):
    num_seq = pieces.num_seq
    rows, width = x_rows.shape
    size = rows // chunks
    half = width // 2
    per = chunks // num_seq
    last = n_tp - 1
    z = lax.axis_index('tp')
    z_rows = z * size
    out = jnp.zeros((rows, width), jnp.bfloat16)

    def part(step, index, which):
        lo, hi = max(step - last, 0) // per, min(step, chunks - 1) // per
        pick = None
        for n in range(lo, hi + 1):
            at = index - n * per * size
            piece = lax.dynamic_slice(partials[n][which], (at, 0), (size, half), allow_negative_indices=False)
            pick = piece if pick is None else jnp.where(at >= 0, piece, pick)
        return pick

    def send(value, step, up, live):
        pairs = []
        for d in range(n_tp):
            to = d + 1 if up else d - 1
            if 0 <= to < n_tp and 0 <= live(d, step) < chunks:
                pairs.append((d, to))
        if not pairs:
            return None
        return lax.ppermute(value, 'tp', pairs)

    sum_up = sum_dn = None
    got_b = got_a = None
    fin_b = fin_a = None
    keep_b = keep_a = None
    for t in range(chunks + 2 * last + 1):
        moving = t < chunks + last
        returning = 0 <= t - 1 - last and t - 1 - 2 * last < chunks
        up = dn = val_b = val_a = None
        if returning:
            base_b = t - 1 - 2 * last
            base_a = t - 1 - last
            val_b = fin_b if got_b is None else (got_b if fin_b is None else jnp.where(z == last, fin_b, got_b))
            val_a = fin_a if got_a is None else (got_a if fin_a is None else jnp.where(z == 0, fin_a, got_a))
        if moving:
            up = part(t, t * size - z_rows, 1)
            dn = part(t, (t - last) * size + z_rows, 0)
            if sum_up is not None:
                up = up + jnp.where(z == 0, 0.0, sum_up)
                dn = dn + jnp.where(z == last, 0.0, sum_dn)
        gates = [v for v in (up, dn, val_b, val_a) if v is not None]
        if moving:
            gates.append(x_rows)
            gates = list(pieces.open(gates) if pieces.left() else together(*gates))
            x_rows = gates.pop()
        if moving:
            up, dn = gates[:2]
            gates = gates[2:]
        if returning:
            val_b, val_a = gates
        next_up = next_dn = next_b = next_a = None
        if moving:
            next_up = send(up, t, True, lambda d, s: s - d)
            next_dn = send(dn, t, False, lambda d, s: s - last + d)
        if returning:
            next_b = send(val_b, t, False, lambda d, s: s - 1 - 2 * last + d)
            next_a = send(val_a, t, True, lambda d, s: s - 1 - last - d)
            idx_b = base_b * size + z_rows
            idx_a = base_a * size - z_rows
            if t - 1 - last >= chunks:
                val_b = jnp.where(idx_b < rows, val_b, keep_b)
                val_a = jnp.where(idx_a < rows, val_a, keep_a)
            keep_b, keep_a = val_b, val_a
            out = lax.dynamic_update_slice(out, val_b, (idx_b, half), allow_negative_indices=False)
            out = lax.dynamic_update_slice(out, val_a, (idx_a, 0), allow_negative_indices=False)
        fin_b = fin_a = None
        if moving and t >= last:
            x_piece = lax.slice(x_rows, ((t - last) * size, 0), ((t - last + 1) * size, width)).astype(jnp.float32)
            fin_b = (x_piece[:, half:] + up).astype(jnp.bfloat16)
            fin_a = (x_piece[:, :half] + dn).astype(jnp.bfloat16)
        if pieces.left():
            done = [v for v in (next_up, next_dn, next_b, next_a) if v is not None]
            done = iter(pieces.close(done))
            next_up, next_dn, next_b, next_a = [None if v is None else next(done)
                                                for v in (next_up, next_dn, next_b, next_a)]
        sum_up, sum_dn, got_b, got_a = next_up, next_dn, next_b, next_a
    return out


class Pieces:
    def __init__(self, steps, first, num_seq):
        self.steps = list(steps)
        self.state = first
        self.num_seq = num_seq
        self.at = 0

    def left(self):
        return self.at < len(self.steps)

    def open(self, gates):
        tied = together(*self.state, *gates)
        count = len(self.state)
        self.state = tuple(self.steps[self.at](*tied[:count]))
        return tied[count:]

    def close(self, done):
        tied = together(*self.state, *done)
        self.state = tuple(tied[:len(self.state)])
        self.at += 1
        return tied[len(self.state):]


def solution(mesh):
    n_tp = mesh.shape['tp']
    n_cp = mesh.shape['cp']

    def local_block(x_blk, pos_blk, w_dq, g_q, w_uq, w_dkv, g_kv, w_uk, w_uv, w_o):
        num_seq, seq_dev, width = x_blk.shape
        kv_rank = g_kv.shape[0]
        rope_dim = w_dkv.shape[1] - kv_rank
        heads_dev = (w_uq.shape[1] - w_uk.shape[1]) // rope_dim
        nope_dim = w_uk.shape[1] // heads_dev
        soft_scale = (nope_dim + rope_dim) ** -0.5
        n_blocks = 2 * n_cp
        block_len = seq_dev // 2
        n_pairs = heads_dev // PAIR
        cuts = [n_pairs * i // SPLITS for i in range(SPLITS + 1)]
        pos_f32 = pos_blk.astype(jnp.float32)
        x_flat = x_blk.reshape(num_seq * seq_dev, width)
        latents, ropes, tables, gathered, orders = {}, {}, {}, {}, {}
        partials = []

        def compress(rows, pos_rows, prompts):
            cos_t, sin_t = rope_tables(pos_rows, rope_dim)
            kv_joint = jnp.dot(rows, w_dkv, preferred_element_type=jnp.float32).astype(jnp.bfloat16)
            latent = rms_norm(kv_joint[:, :kv_rank], g_kv)
            k_rope = rotate(kv_joint[:, kv_rank:], cos_t, sin_t)
            block_ids = jnp.broadcast_to(jnp.floor(pos_rows / block_len)[:, None].astype(jnp.bfloat16), k_rope.shape)
            both = jnp.concatenate([latent, k_rope, block_ids], axis=1)
            both = both.reshape(len(prompts), seq_dev, -1)
            both_all = lax.all_gather(both, 'cp', axis=1, tiled=True)
            cos2 = jnp.concatenate([cos_t, cos_t], axis=1).reshape(len(prompts), seq_dev, rope_dim)
            sin2 = jnp.concatenate([-sin_t, sin_t], axis=1).reshape(len(prompts), seq_dev, rope_dim)
            for i, n in enumerate(prompts):
                latents[n] = latent[i * seq_dev:(i + 1) * seq_dev]
                ropes[n] = k_rope[i * seq_dev:(i + 1) * seq_dev]
                tables[n] = (cos2[i], sin2[i])
                gathered[n] = both_all[i].reshape(n_blocks, block_len, -1)

        def order_of(n):
            ids_all = gathered[n][:, 0, kv_rank + rope_dim].astype(jnp.int32)
            blocks = jnp.arange(n_blocks, dtype=jnp.int32)
            where = jnp.sum(jnp.where(ids_all[None, :] == blocks[:, None], blocks[None, :], 0), axis=1)
            return jnp.concatenate([where, pos_blk[n, :1] // block_len]).astype(jnp.int32)

        def q_down(rows):
            return jnp.dot(rows, w_dq, preferred_element_type=jnp.float32).astype(jnp.bfloat16)

        def q_up(q_latent):
            return jnp.dot(rms_norm(q_latent, g_q), w_uq, preferred_element_type=jnp.float32).astype(jnp.bfloat16)

        def heads_of(n, q_full, pairs, prior):
            return attend(q_full, *tables[n], gathered[n], orders[n], w_uk, w_uv, heads_dev, soft_scale, pairs, prior)

        def product(attn, which):
            cols = w_o.shape[1] // 2
            return jnp.dot(attn, w_o[:, which * cols:(which + 1) * cols], preferred_element_type=jnp.float32)

        def later(n):
            rows = slice(n * seq_dev, (n + 1) * seq_dev)

            def step_down(x_all):
                return x_all, q_down(x_all[rows])

            def step_up(x_all, q_latent):
                if n not in orders:
                    orders[n] = order_of(n)
                return x_all, q_up(q_latent)

            def step_attend(i, x_all, q_full, *prior):
                attn = heads_of(n, q_full, range(cuts[i], cuts[i + 1]), prior[0] if prior else None)
                return (x_all, q_full, attn) if i + 1 < SPLITS else (x_all, attn)

            def step_second(x_all, attn):
                return x_all, attn, product(attn, 1)

            def step_first(x_all, attn, second):
                partials.append((product(attn, 0), second))
                return x_all, *partials[-1]

            def step_settle(x_all, first, second):
                partials[n] = (first, second)
                return (x_all,)

            return ([step_down, step_up] + [functools.partial(step_attend, i) for i in range(SPLITS)]
                    + [step_second, step_first], step_settle)

        compress(x_flat[:seq_dev], pos_f32[0], [0])
        q_full = q_up(q_down(x_flat[:seq_dev]))
        orders[0] = order_of(0)
        attn = heads_of(0, q_full, range(n_pairs), None)
        partials.append((product(attn, 0), product(attn, 1)))

        def step_compress(x_all):
            rest = list(range(1, num_seq))
            compress(x_all[seq_dev:], pos_f32[1:].reshape(-1), rest)
            return x_all, jnp.concatenate([latents[n] for n in rest])

        steps = [step_compress]
        first_state = (x_flat,)
        chain = []
        for n in range(1, num_seq):
            work, settle = later(n)
            chain.append((work, settle))
        steps = [step_compress]
        pending = lambda x_all, *_: (x_all,)
        for work, settle in chain:
            head = functools.partial(lambda before, fn, *state: fn(*before(*state)), pending, work[0])
            steps += [head] + work[1:]
            pending = settle
        pieces = Pieces(steps, first_state, num_seq)
        out = chain_sum(partials, pieces, x_flat, n_tp, CHUNKS)
        out = out.reshape(x_blk.shape)
        return (out, jnp.stack([latents[n] for n in range(num_seq)]), jnp.stack([ropes[n] for n in range(num_seq)]))

    seq_spec = P('dp', 'cp', None)
    in_specs = (seq_spec, P('dp', 'cp'), P(None, None), P(None), P(None, 'tp'), P(None, None), P(None),
                P(None, 'tp'), P(None, 'tp'), P('tp', None))
    return jax.shard_map(local_block, mesh=mesh, in_specs=in_specs,
                         out_specs=(seq_spec, seq_spec, seq_spec), check_vma=False)
```

```python
import functools

import jax
import jax.numpy as jnp
from jax import lax
from jax.experimental import pallas as pl
from jax.experimental.pallas import tpu as pltpu
from jax.sharding import PartitionSpec as P

ROPE_BASE = 10000.0
NORM_EPS = 1e-6
LOG2_E = 1.4426950408889634
CHUNK = 32
LAG = 2
LAG_BACK = 2
PAIR = 2
SPLITS = 3


def rms_norm(tensor, norm_gain):
    tensor_f32 = tensor.astype(jnp.float32)
    inv_rms = lax.rsqrt(jnp.mean(tensor_f32 * tensor_f32, axis=-1, keepdims=True) + NORM_EPS)
    return (tensor_f32 * inv_rms * norm_gain).astype(jnp.bfloat16)


def rope_tables(positions, rope_dim):
    inv_freq = ROPE_BASE ** (-2.0 * jnp.arange(rope_dim // 2, dtype=jnp.float32) / rope_dim)
    angles = positions.astype(jnp.float32)[..., None] * inv_freq
    return jnp.cos(angles), jnp.sin(angles)


def rotate(tensor, cos_t, sin_t):
    tensor_f32 = tensor.astype(jnp.float32)
    half_dim = tensor_f32.shape[-1] // 2
    lower_half = tensor_f32[..., :half_dim]
    upper_half = tensor_f32[..., half_dim:]
    return jnp.concatenate([lower_half * cos_t - upper_half * sin_t,
                            lower_half * sin_t + upper_half * cos_t], axis=-1).astype(jnp.bfloat16)


def attend_kernel(soft_scale, row, order_ref, q_ref, cos_ref, sin_ref, lat_hbm, w_uk_ref, w_uv_ref, *rest):
    o_ref, lat_s, sems = rest[-3:]
    n_blocks, block_len = lat_hbm.shape[1:3]
    half_keys = n_blocks // 2 * block_len
    rank = w_uk_ref.shape[0]
    rope_dim = cos_ref.shape[1]
    nope_dim = w_uk_ref.shape[1] // PAIR
    v_dim = w_uv_ref.shape[1] // PAIR
    qk_dim = nope_dim + rope_dim

    @pl.when(pl.program_id(0) == 0)
    def _():
        copies = [pltpu.make_async_copy(lat_hbm.at[row, order_ref[j]], lat_s.at[pl.ds(j * block_len, block_len)],
                                        sems.at[j])
                  for j in range(n_blocks)]
        for copy in copies:
            copy.start()
        for copy in copies:
            copy.wait()

    low_id = order_ref[n_blocks]
    latent = lat_s[:, :rank]
    k_rope = lat_s[:, rank:rank + rope_dim]
    k_pair = jnp.dot(latent, w_uk_ref[...], preferred_element_type=jnp.float32).astype(jnp.bfloat16)
    v_pair = jnp.dot(latent, w_uv_ref[...], preferred_element_type=jnp.float32).astype(jnp.bfloat16)

    q_pair = q_ref[...].astype(jnp.float32)
    cos2 = cos_ref[...]
    sin2 = sin_ref[...]
    col_minus_row = (lax.broadcasted_iota(jnp.int32, (block_len, half_keys), 1)
                     - lax.broadcasted_iota(jnp.int32, (block_len, half_keys), 0))
    low_mask = col_minus_row <= low_id * block_len
    high_mask = col_minus_row <= (n_blocks - 1 - low_id) * block_len - half_keys
    factor = soft_scale * LOG2_E
    contract_last = (((1,), (1,)), ((), ()))

    for head in range(PAIR):
        q_head = q_pair if head == 0 else pltpu.roll(q_pair, (PAIR - head) * qk_dim, 1)
        q_rope = q_head[:, nope_dim:qk_dim]
        swapped = jnp.concatenate([q_rope[:, rope_dim // 2:], q_rope[:, :rope_dim // 2]], axis=1)
        q_rot = q_rope * cos2 + swapped * sin2
        q_cat = jnp.concatenate([q_head[:, :nope_dim], q_rot], axis=1).astype(jnp.bfloat16)
        k_cat = jnp.concatenate([k_pair[:, head * nope_dim:(head + 1) * nope_dim], k_rope], axis=1)
        v_head = v_pair[:, head * v_dim:(head + 1) * v_dim]
        early = lax.dot_general(q_cat, k_cat[:half_keys], contract_last, preferred_element_type=jnp.float32)
        late = lax.dot_general(q_cat[block_len:], k_cat[half_keys:], contract_last,
                               preferred_element_type=jnp.float32)

        low = jnp.where(low_mask, early[:block_len], -jnp.inf)
        low_exp = jnp.exp2((low - jnp.max(low, axis=1, keepdims=True)) * factor)
        low_prob = (low_exp * (1.0 / jnp.sum(low_exp, axis=1, keepdims=True))).astype(jnp.bfloat16)
        low_out = jnp.dot(low_prob, v_head[:half_keys], preferred_element_type=jnp.float32)

        near = early[block_len:]
        far = jnp.where(high_mask, late, -jnp.inf)
        top = jnp.maximum(jnp.max(near, axis=1, keepdims=True), jnp.max(far, axis=1, keepdims=True))
        near_exp = jnp.exp2((near - top) * factor)
        far_exp = jnp.exp2((far - top) * factor)
        inv_sum = 1.0 / (jnp.sum(near_exp, axis=1, keepdims=True) + jnp.sum(far_exp, axis=1, keepdims=True))
        high_out = (jnp.dot((near_exp * inv_sum).astype(jnp.bfloat16), v_head[:half_keys],
                            preferred_element_type=jnp.float32)
                    + jnp.dot((far_exp * inv_sum).astype(jnp.bfloat16), v_head[half_keys:],
                              preferred_element_type=jnp.float32))
        o_ref[:block_len, head * v_dim:(head + 1) * v_dim] = low_out.astype(jnp.bfloat16)
        o_ref[block_len:, head * v_dim:(head + 1) * v_dim] = high_out.astype(jnp.bfloat16)


def attend(q_full, cos2, sin2, lat_blocks, order, w_uk, w_uv, heads, soft_scale, row, prompt, pairs, prior):
    n_rows, n_blocks, block_len, width = lat_blocks.shape
    tokens = q_full.shape[0] // n_rows
    rank = w_uk.shape[0]
    keys = n_blocks * block_len
    qk_dim = q_full.shape[1] // heads
    nope_dim = w_uk.shape[1] // heads
    v_dim = w_uv.shape[1] // heads
    rope_dim = cos2.shape[1]
    first, count = pairs[0], len(pairs)
    flops = (2 * keys * rank * (nope_dim + v_dim) + 2 * tokens * keys * 3 // 4 * (qk_dim + v_dim)) * count * PAIR
    moved = 2 * (lat_blocks.size // n_rows + (tokens * (qk_dim + v_dim) + rank * (nope_dim + v_dim)) * count * PAIR)
    in_specs = [
        pl.BlockSpec((tokens, PAIR * qk_dim), lambda h, order: (row, h + first)),
        pl.BlockSpec((tokens, rope_dim), lambda h, order: (prompt, 0)),
        pl.BlockSpec((tokens, rope_dim), lambda h, order: (prompt, 0)),
        pl.BlockSpec(memory_space=pl.ANY),
        pl.BlockSpec((rank, PAIR * nope_dim), lambda h, order: (0, h + first)),
        pl.BlockSpec((rank, PAIR * v_dim), lambda h, order: (0, h + first)),
    ]
    operands = [q_full, cos2, sin2, lat_blocks, w_uk, w_uv]
    aliases = {}
    if prior is not None:
        in_specs.append(pl.BlockSpec(memory_space=pl.ANY))
        operands.append(prior)
        aliases = {len(operands): 0}
    return pl.pallas_call(
        functools.partial(attend_kernel, soft_scale, row),
        out_shape=jax.ShapeDtypeStruct((n_rows * tokens, heads * v_dim), jnp.bfloat16),
        grid_spec=pltpu.PrefetchScalarGridSpec(
            num_scalar_prefetch=1,
            grid=(count,),
            in_specs=in_specs,
            out_specs=pl.BlockSpec((tokens, PAIR * v_dim), lambda h, order: (row, h + first)),
            scratch_shapes=[pltpu.VMEM((keys, width), jnp.bfloat16), pltpu.SemaphoreType.DMA((n_blocks,))],
        ),
        input_output_aliases=aliases,
        compiler_params=pltpu.CompilerParams(dimension_semantics=("arbitrary",), vmem_limit_bytes=56 * 1024 * 1024),
        cost_estimate=pl.CostEstimate(flops=flops, bytes_accessed=moved,
                                      transcendentals=tokens * keys * count * PAIR * 3 // 4),
        name="attend",
    )(order, *operands)


def together(*values):
    return lax.optimization_barrier(values)


def chain_kernel(n_tp, size, attn, w_o, x_rows, out, got_up, got_dn, w_v, a_v, p_v, r_v, x_v, f_v,
                 w_sem, a_sem, r_sem, x_sem, f_sem, sum_sent, sum_got, res_sent, res_got):
    z = lax.axis_index('tp')
    last = n_tp - 1
    half = out.shape[1] // 2
    chunks = attn.shape[0] // size
    skip = out.shape[0] - attn.shape[0]
    got = (got_up, got_dn)
    place = (z, last - z)
    ahead = (z + 1, z - 1)
    behind = (z - 1, z + 1)
    first_col = (half, 0)
    tile = w_v.shape[1] // w_sem.shape[0]

    barrier = pltpu.get_barrier_semaphore()
    for there, device in ((z > 0, z - 1), (z < last, z + 1)):
        @pl.when(there)
        def _():
            pl.semaphore_signal(barrier, inc=1, device_id={'tp': device}, device_id_type=pl.DeviceIdType.MESH)
    middle = (z > 0) & (z < last)

    @pl.when(middle)
    def _():
        pl.semaphore_wait(barrier, 2)

    @pl.when(jnp.logical_not(middle))
    def _():
        pl.semaphore_wait(barrier, 1)

    def w_copy(i):
        cols = pl.ds(i * tile, tile)
        return pltpu.make_async_copy(w_o.at[:, cols], w_v.at[:, cols], w_sem.at[i])

    tiles = w_sem.shape[0]
    for i in range(tiles // 2):
        w_copy(i).start()
        w_copy(tiles // 2 + i).start()

    def rows_of(u):
        return pl.ds(pl.multiple_of(u * size, size), size)

    def out_rows(u):
        return pl.ds(pl.multiple_of(skip + u * size, size), size)

    def a_copy(d, u):
        slot = lax.rem(u, 2)
        return pltpu.make_async_copy(attn.at[rows_of(u)], a_v.at[d, slot], a_sem.at[d, slot])

    def r_copy(d, u):
        return pltpu.make_async_copy(got[d].at[rows_of(u)], r_v.at[d], r_sem.at[d])

    def x_copy(d, u):
        return pltpu.make_async_copy(x_rows.at[out_rows(u), pl.ds(first_col[d], half)], x_v.at[d], x_sem.at[d])

    def f_copy(d, u):
        slot = lax.rem(u, 2)
        return pltpu.make_async_copy(f_v.at[d, slot], out.at[out_rows(u), pl.ds(first_col[d], half)],
                                     f_sem.at[d, slot])

    def sum_send(d, u):
        return pltpu.make_async_remote_copy(
            src_ref=p_v.at[d, lax.rem(u, 2)], dst_ref=got[d].at[rows_of(u)],
            send_sem=sum_sent.at[d, u], recv_sem=sum_got.at[d, u],
            device_id={'tp': ahead[d]}, device_id_type=pl.DeviceIdType.MESH)

    def res_first(d, u):
        return pltpu.make_async_remote_copy(
            src_ref=f_v.at[d, lax.rem(u, 2)], dst_ref=out.at[out_rows(u), pl.ds(first_col[d], half)],
            send_sem=res_sent.at[d, u], recv_sem=res_got.at[d, u],
            device_id={'tp': behind[d]}, device_id_type=pl.DeviceIdType.MESH)

    def res_pass(d, u):
        here = out.at[out_rows(u), pl.ds(first_col[d], half)]
        return pltpu.make_async_remote_copy(
            src_ref=here, dst_ref=here, send_sem=res_sent.at[d, u], recv_sem=res_got.at[d, u],
            device_id={'tp': behind[d]}, device_id_type=pl.DeviceIdType.MESH)

    def inside(u):
        return (u >= 0) & (u < chunks)

    def step(index, carry):
        t = index - 2
        chunk = [t - LAG * place[d] for d in range(2)]
        for d in range(2):
            u = chunk[d]

            @pl.when(inside(u) & (place[d] > 0))
            def _():
                sum_send(d, u).wait_recv()
                r_copy(d, u).start()

            @pl.when(inside(u) & (place[d] == last))
            def _():
                x_copy(d, u).start()

        for d in range(2):
            u = chunk[d]
            slot = lax.rem(u + 2, 2)

            @pl.when(inside(u) & (place[d] > 0))
            def _():
                r_copy(d, u).wait()

            @pl.when(inside(u) & (place[d] > 0) & (place[d] < last))
            def _():
                p_v[d, slot] = p_v[d, slot] + r_v[d]

            @pl.when(inside(u) & (place[d] < last))
            def _():
                sum_send(d, u).start()

            @pl.when(inside(u) & (place[d] == last))
            def _():
                x_copy(d, u).wait()
                f_v[d, slot] = (x_v[d].astype(jnp.float32) + (p_v[d, slot] + r_v[d])).astype(jnp.bfloat16)
                f_copy(d, u).start()
                res_first(d, u).start()

        for d in range(2):
            v = t - LAG * last - LAG_BACK * (last - place[d])

            @pl.when(inside(v) & (place[d] > 0) & (place[d] < last))
            def _():
                res_pass(d, v).wait_recv()
                res_pass(d, v).start()

        @pl.when(t == -1)
        def _():
            for i in range(tiles):
                w_copy(i).wait()

        for d in range(2):
            u = chunk[d]

            @pl.when(inside(u + 2))
            def _():
                a_copy(d, u + 2).start()

            @pl.when(inside(u + 1))
            def _():
                slot = lax.rem(u + 1, 2)

                @pl.when(inside(u - 1) & (place[d] < last))
                def _():
                    sum_send(d, u - 1).wait_send()

                @pl.when(inside(u - 1) & (place[d] == last))
                def _():
                    f_copy(d, u - 1).wait()
                    res_first(d, u - 1).wait_send()

                a_copy(d, u + 1).wait()

                def column_tile(j, carry):
                    cols = pl.ds(pl.multiple_of(j * tile, tile), tile)
                    w_cols = pl.ds(pl.multiple_of(first_col[d] + j * tile, tile), tile)
                    p_v[d, slot, :, cols] = jnp.dot(a_v[d, slot], w_v[:, w_cols], preferred_element_type=jnp.float32)
                    return carry

                lax.fori_loop(0, tiles // 2, column_tile, 0)
        return carry

    lax.fori_loop(0, chunks + 2 + LAG * last + LAG_BACK * (last - 1), step, 0)

    for d in range(2):
        for u in (chunks - 2, chunks - 1):
            @pl.when(place[d] < last)
            def _():
                sum_send(d, u).wait_send()

            @pl.when(place[d] == last)
            def _():
                f_copy(d, u).wait()
                res_first(d, u).wait_send()

        def drain(u, carry):
            @pl.when((place[d] > 0) & (place[d] < last))
            def _():
                res_pass(d, u).wait_send()

            @pl.when(place[d] == 0)
            def _():
                res_pass(d, u).wait_recv()
            return carry

        lax.fori_loop(0, chunks, drain, 0)


def chain_sum(attn, w_o, x_rows, n_tp, size):
    rows, inner = attn.shape
    width = w_o.shape[1]
    half = width // 2
    chunks = rows // size
    tiles = 2 * max(1, half // 512)
    sems = pltpu.SemaphoreType.DMA
    out, _, _ = pl.pallas_call(
        functools.partial(chain_kernel, n_tp, size),
        out_shape=(jax.ShapeDtypeStruct(x_rows.shape, jnp.bfloat16),
                   jax.ShapeDtypeStruct((rows, half), jnp.float32),
                   jax.ShapeDtypeStruct((rows, half), jnp.float32)),
        in_specs=[pl.BlockSpec(memory_space=pl.ANY)] * 3,
        out_specs=(pl.BlockSpec(memory_space=pl.ANY),) * 3,
        scratch_shapes=[
            pltpu.VMEM((inner, width), jnp.bfloat16),
            pltpu.VMEM((2, 2, size, inner), jnp.bfloat16),
            pltpu.VMEM((2, 2, size, half), jnp.float32),
            pltpu.VMEM((2, size, half), jnp.float32),
            pltpu.VMEM((2, size, half), jnp.bfloat16),
            pltpu.VMEM((2, 2, size, half), jnp.bfloat16),
            sems((tiles,)), sems((2, 2)), sems((2,)), sems((2,)), sems((2, 2)),
            sems((2, chunks)), sems((2, chunks)), sems((2, chunks)), sems((2, chunks)),
        ],
        compiler_params=pltpu.CompilerParams(collective_id=0, has_side_effects=True,
                                             vmem_limit_bytes=60 * 1024 * 1024),
        cost_estimate=pl.CostEstimate(flops=2 * rows * inner * width, transcendentals=0,
                                      bytes_accessed=2 * inner * width + 12 * rows * width),
        name="chain_sum",
    )(attn, w_o, x_rows)
    return out


def solution(mesh):
    n_tp = mesh.shape['tp']
    n_cp = mesh.shape['cp']

    def local_step(x_blk, pos_blk, w_dq, g_q, w_uq, w_dkv, g_kv, w_uk, w_uv, w_o):
        num_seq, seq_dev, width = x_blk.shape
        kv_rank = g_kv.shape[0]
        rope_dim = w_dkv.shape[1] - kv_rank
        heads_dev = (w_uq.shape[1] - w_uk.shape[1]) // rope_dim
        nope_dim = w_uk.shape[1] // heads_dev
        soft_scale = (nope_dim + rope_dim) ** -0.5
        n_blocks = 2 * n_cp
        block_len = seq_dev // 2
        n_pairs = heads_dev // PAIR
        cuts = [n_pairs * i // SPLITS for i in range(SPLITS + 1)]
        pos_f32 = pos_blk.astype(jnp.float32)
        x_flat = x_blk.reshape(num_seq * seq_dev, width)

        cos_t, sin_t = rope_tables(pos_f32.reshape(-1), rope_dim)
        tables = (jnp.concatenate([cos_t, cos_t], axis=1), jnp.concatenate([-sin_t, sin_t], axis=1))
        kv_joint = jnp.dot(x_flat, w_dkv, preferred_element_type=jnp.float32).astype(jnp.bfloat16)
        latent = rms_norm(kv_joint[:, :kv_rank], g_kv)
        k_rope = rotate(kv_joint[:, kv_rank:], cos_t, sin_t)
        block_ids = jnp.floor(pos_f32.reshape(-1) / block_len)[:, None].astype(jnp.bfloat16)
        both = jnp.concatenate([latent, k_rope, jnp.broadcast_to(block_ids, k_rope.shape)], axis=1)
        both = both.reshape(num_seq, seq_dev, -1)

        def gather(lo, hi):
            everyone = lax.all_gather(both[lo:hi], 'cp', axis=1, tiled=True).reshape(hi - lo, n_blocks, block_len, -1)
            ids_all = everyone[:, :, 0, kv_rank + rope_dim].astype(jnp.int32)
            blocks = jnp.arange(n_blocks, dtype=jnp.int32)
            where = jnp.sum(jnp.where(ids_all[:, None, :] == blocks[:, None], blocks, 0), axis=2)
            order = jnp.concatenate([where, pos_blk[lo:hi, :1] // block_len], axis=1).astype(jnp.int32)
            return everyone, order

        def q_of(rows):
            q_latent = jnp.dot(rows, w_dq, preferred_element_type=jnp.float32).astype(jnp.bfloat16)
            return jnp.dot(rms_norm(q_latent, g_q), w_uq, preferred_element_type=jnp.float32).astype(jnp.bfloat16)

        x_first, x_rest = x_flat[:seq_dev], x_flat[seq_dev:]
        everyone, order = gather(0, 1)
        everyone_r, order_r = gather(1, num_seq)
        attn = attend(q_of(x_first), *tables, everyone, order[0], w_uk, w_uv, heads_dev, soft_scale, 0, 0,
                      range(n_pairs), None)
        share = jnp.dot(attn, w_o, preferred_element_type=jnp.float32)
        x_rest, share = together(x_rest, share)
        mine = lax.psum_scatter(share, 'tp', scatter_dimension=0, tiled=True)
        q_rest = q_of(x_rest)
        attn = None
        for n in range(num_seq - 1):
            for i in range(SPLITS):
                attn = attend(q_rest, *tables, everyone_r, order_r[n], w_uk, w_uv, heads_dev, soft_scale, n, n + 1,
                              range(cuts[i], cuts[i + 1]), attn)
                if n == num_seq - 2 and i == 0:
                    attn, mine = together(attn, mine)
                    own = mine.shape[0]
                    x_own = lax.dynamic_slice(x_first, (lax.axis_index('tp') * own, 0), (own, width))
                    first_own = (x_own.astype(jnp.float32) + mine).astype(jnp.bfloat16)
                    out_first = lax.all_gather(first_own, 'tp', axis=0, tiled=True)
        out = chain_sum(attn, w_o, x_flat, n_tp, CHUNK)
        out = lax.dynamic_update_slice(out, out_first, (0, 0)).reshape(x_blk.shape)
        return out, latent.reshape(num_seq, seq_dev, -1), k_rope.reshape(num_seq, seq_dev, -1)

    seq_spec = P('dp', 'cp', None)
    in_specs = (seq_spec, P('dp', 'cp'), P(None, None), P(None), P(None, 'tp'), P(None, None), P(None),
                P(None, 'tp'), P(None, 'tp'), P('tp', None))
    return jax.shard_map(local_step, mesh=mesh, in_specs=in_specs,
                         out_specs=(seq_spec, seq_spec, seq_spec), check_vma=False)
```

```python
import functools

import jax
import jax.numpy as jnp
from jax import lax
from jax.experimental import pallas as pl
from jax.experimental.pallas import tpu as pltpu
from jax.sharding import PartitionSpec as P

ROPE_BASE = 10000.0
NORM_EPS = 1e-6
LOG2_E = 1.4426950408889634
CHUNK = 32
LAG = 2
LAG_BACK = 2
PAIR = 2


def rms_norm(tensor, norm_gain):
    tensor_f32 = tensor.astype(jnp.float32)
    inv_rms = lax.rsqrt(jnp.mean(tensor_f32 * tensor_f32, axis=-1, keepdims=True) + NORM_EPS)
    return (tensor_f32 * inv_rms * norm_gain).astype(jnp.bfloat16)


def rope_tables(positions, rope_dim):
    inv_freq = ROPE_BASE ** (-2.0 * jnp.arange(rope_dim // 2, dtype=jnp.float32) / rope_dim)
    angles = positions.astype(jnp.float32)[..., None] * inv_freq
    return jnp.cos(angles), jnp.sin(angles)


def rotate(tensor, cos_t, sin_t):
    tensor_f32 = tensor.astype(jnp.float32)
    half_dim = tensor_f32.shape[-1] // 2
    lower_half = tensor_f32[..., :half_dim]
    upper_half = tensor_f32[..., half_dim:]
    return jnp.concatenate([lower_half * cos_t - upper_half * sin_t,
                            lower_half * sin_t + upper_half * cos_t], axis=-1).astype(jnp.bfloat16)


def attend_kernel(soft_scale, row, order_ref, q_ref, cos_ref, sin_ref, lat_hbm, w_uk_ref, w_uv_ref, *rest):
    o_ref, lat_s, sems = rest[-3:]
    n_blocks, block_len = lat_hbm.shape[1:3]
    half_keys = n_blocks // 2 * block_len
    rank = w_uk_ref.shape[0]
    rope_dim = cos_ref.shape[1]
    nope_dim = w_uk_ref.shape[1] // PAIR
    v_dim = w_uv_ref.shape[1] // PAIR
    qk_dim = nope_dim + rope_dim

    @pl.when(pl.program_id(0) == 0)
    def _():
        copies = [pltpu.make_async_copy(lat_hbm.at[row, order_ref[j]], lat_s.at[pl.ds(j * block_len, block_len)],
                                        sems.at[j])
                  for j in range(n_blocks)]
        for copy in copies:
            copy.start()
        for copy in copies:
            copy.wait()

    low_id = order_ref[n_blocks]
    latent = lat_s[:, :rank]
    k_rope = lat_s[:, rank:rank + rope_dim]
    k_pair = jnp.dot(latent, w_uk_ref[...], preferred_element_type=jnp.float32).astype(jnp.bfloat16)

    q_pair = q_ref[...].astype(jnp.float32)
    cos2 = cos_ref[...]
    sin2 = sin_ref[...]
    col_minus_row = (lax.broadcasted_iota(jnp.int32, (block_len, half_keys), 1)
                     - lax.broadcasted_iota(jnp.int32, (block_len, half_keys), 0))
    low_mask = col_minus_row <= low_id * block_len
    high_mask = col_minus_row <= (n_blocks - 1 - low_id) * block_len - half_keys
    factor = soft_scale * LOG2_E
    contract_last = (((1,), (1,)), ((), ()))

    def scores(head):
        q_head = q_pair if head == 0 else pltpu.roll(q_pair, (PAIR - head) * qk_dim, 1)
        q_rope = q_head[:, nope_dim:qk_dim]
        swapped = jnp.concatenate([q_rope[:, rope_dim // 2:], q_rope[:, :rope_dim // 2]], axis=1)
        q_rot = q_rope * cos2 + swapped * sin2
        q_cat = jnp.concatenate([q_head[:, :nope_dim], q_rot], axis=1).astype(jnp.bfloat16)
        k_cat = jnp.concatenate([k_pair[:, head * nope_dim:(head + 1) * nope_dim], k_rope], axis=1)
        early = lax.dot_general(q_cat, k_cat[:half_keys], contract_last, preferred_element_type=jnp.float32)
        late = lax.dot_general(q_cat[block_len:], k_cat[half_keys:], contract_last,
                               preferred_element_type=jnp.float32)
        return early, late

    def low_probs(early):
        low = jnp.where(low_mask, early[:block_len], -jnp.inf)
        low_exp = jnp.exp2((low - jnp.max(low, axis=1, keepdims=True)) * factor)
        return (low_exp * (1.0 / jnp.sum(low_exp, axis=1, keepdims=True))).astype(jnp.bfloat16)

    def high_probs(early, late):
        near = early[block_len:]
        far = jnp.where(high_mask, late, -jnp.inf)
        top = jnp.maximum(jnp.max(near, axis=1, keepdims=True), jnp.max(far, axis=1, keepdims=True))
        near_exp = jnp.exp2((near - top) * factor)
        far_exp = jnp.exp2((far - top) * factor)
        inv_sum = 1.0 / (jnp.sum(near_exp, axis=1, keepdims=True) + jnp.sum(far_exp, axis=1, keepdims=True))
        return (near_exp * inv_sum).astype(jnp.bfloat16), (far_exp * inv_sum).astype(jnp.bfloat16)

    def low_value(head, probs):
        cols = slice(head * v_dim, (head + 1) * v_dim)
        o_ref[:block_len, cols] = jnp.dot(probs, v_pair[:half_keys, cols],
                                          preferred_element_type=jnp.float32).astype(jnp.bfloat16)

    def high_value(head, near, far):
        cols = slice(head * v_dim, (head + 1) * v_dim)
        o_ref[block_len:, cols] = (jnp.dot(near, v_pair[:half_keys, cols], preferred_element_type=jnp.float32)
                                   + jnp.dot(far, v_pair[half_keys:, cols],
                                             preferred_element_type=jnp.float32)).astype(jnp.bfloat16)

    first = scores(0)
    v_pair = jnp.dot(latent, w_uv_ref[...], preferred_element_type=jnp.float32).astype(jnp.bfloat16)
    low = low_probs(first[0])
    second = scores(1)
    high = high_probs(*first)
    low_value(0, low)
    low = low_probs(second[0])
    high_value(0, *high)
    high = high_probs(*second)
    low_value(1, low)
    high_value(1, *high)


def attend(q_full, cos2, sin2, lat_blocks, order, w_uk, w_uv, heads, soft_scale, row, prompt, pairs, prior):
    n_rows, n_blocks, block_len, width = lat_blocks.shape
    tokens = q_full.shape[0] // n_rows
    rank = w_uk.shape[0]
    keys = n_blocks * block_len
    qk_dim = q_full.shape[1] // heads
    nope_dim = w_uk.shape[1] // heads
    v_dim = w_uv.shape[1] // heads
    rope_dim = cos2.shape[1]
    first, count = pairs[0], len(pairs)
    flops = (2 * keys * rank * (nope_dim + v_dim) + 2 * tokens * keys * 3 // 4 * (qk_dim + v_dim)) * count * PAIR
    moved = 2 * (lat_blocks.size // n_rows + (tokens * (qk_dim + v_dim) + rank * (nope_dim + v_dim)) * count * PAIR)
    in_specs = [
        pl.BlockSpec((tokens, PAIR * qk_dim), lambda h, order: (row, h + first)),
        pl.BlockSpec((tokens, rope_dim), lambda h, order: (prompt, 0)),
        pl.BlockSpec((tokens, rope_dim), lambda h, order: (prompt, 0)),
        pl.BlockSpec(memory_space=pl.ANY),
        pl.BlockSpec((rank, PAIR * nope_dim), lambda h, order: (0, h + first)),
        pl.BlockSpec((rank, PAIR * v_dim), lambda h, order: (0, h + first)),
    ]
    operands = [q_full, cos2, sin2, lat_blocks, w_uk, w_uv]
    aliases = {}
    if prior is not None:
        in_specs.append(pl.BlockSpec(memory_space=pl.ANY))
        operands.append(prior)
        aliases = {len(operands): 0}
    return pl.pallas_call(
        functools.partial(attend_kernel, soft_scale, row),
        out_shape=jax.ShapeDtypeStruct((n_rows * tokens, heads * v_dim), jnp.bfloat16),
        grid_spec=pltpu.PrefetchScalarGridSpec(
            num_scalar_prefetch=1,
            grid=(count,),
            in_specs=in_specs,
            out_specs=pl.BlockSpec((tokens, PAIR * v_dim), lambda h, order: (row, h + first)),
            scratch_shapes=[pltpu.VMEM((keys, width), jnp.bfloat16), pltpu.SemaphoreType.DMA((n_blocks,))],
        ),
        input_output_aliases=aliases,
        compiler_params=pltpu.CompilerParams(dimension_semantics=("arbitrary",), vmem_limit_bytes=56 * 1024 * 1024),
        cost_estimate=pl.CostEstimate(flops=flops, bytes_accessed=moved,
                                      transcendentals=tokens * keys * count * PAIR * 3 // 4),
        name="attend",
    )(order, *operands)


def together(*values):
    return lax.optimization_barrier(values)


def chain_kernel(n_tp, size, attn, w_o, x_rows, out, got_up, got_dn, w_v, a_v, p_v, r_v, x_v, f_v,
                 w_sem, a_sem, r_sem, x_sem, f_sem, sum_sent, sum_got, res_sent, res_got):
    z = lax.axis_index('tp')
    last = n_tp - 1
    half = out.shape[1] // 2
    chunks = attn.shape[0] // size
    skip = x_rows.shape[0] - attn.shape[0]
    got = (got_up, got_dn)
    place = (z, last - z)
    ahead = (z + 1, z - 1)
    behind = (z - 1, z + 1)
    first_col = (half, 0)
    tile = w_v.shape[1] // w_sem.shape[0]

    barrier = pltpu.get_barrier_semaphore()
    for there, device in ((z > 0, z - 1), (z < last, z + 1)):
        @pl.when(there)
        def _():
            pl.semaphore_signal(barrier, inc=1, device_id={'tp': device}, device_id_type=pl.DeviceIdType.MESH)
    middle = (z > 0) & (z < last)

    @pl.when(middle)
    def _():
        pl.semaphore_wait(barrier, 2)

    @pl.when(jnp.logical_not(middle))
    def _():
        pl.semaphore_wait(barrier, 1)

    def w_copy(i):
        cols = pl.ds(i * tile if isinstance(i, int) else pl.multiple_of(i * tile, tile), tile)
        return pltpu.make_async_copy(w_o.at[:, cols], w_v.at[:, cols], w_sem.at[i])

    tiles = w_sem.shape[0]
    second = list(range(tiles // 2, tiles))
    first = list(range(tiles // 2))
    for near, wanted in ((z <= last // 2, second + first), (z > last // 2, first + second)):
        @pl.when(near)
        def _():
            for i in wanted:
                w_copy(i).start()

    def rows_of(u):
        return pl.ds(pl.multiple_of(u * size, size), size)

    def x_rows_of(u):
        return pl.ds(pl.multiple_of(skip + u * size, size), size)

    def a_copy(d, u):
        slot = lax.rem(u, 2)
        return pltpu.make_async_copy(attn.at[rows_of(u)], a_v.at[d, slot], a_sem.at[d, slot])

    def r_copy(d, u):
        return pltpu.make_async_copy(got[d].at[rows_of(u)], r_v.at[d], r_sem.at[d])

    def x_copy(d, u):
        return pltpu.make_async_copy(x_rows.at[x_rows_of(u), pl.ds(first_col[d], half)], x_v.at[d], x_sem.at[d])

    def f_copy(d, u):
        slot = lax.rem(u, 2)
        return pltpu.make_async_copy(f_v.at[d, slot], out.at[rows_of(u), pl.ds(first_col[d], half)],
                                     f_sem.at[d, slot])

    def sum_send(d, u):
        return pltpu.make_async_remote_copy(
            src_ref=p_v.at[d, lax.rem(u, 2)], dst_ref=got[d].at[rows_of(u)],
            send_sem=sum_sent.at[d, u], recv_sem=sum_got.at[d, u],
            device_id={'tp': ahead[d]}, device_id_type=pl.DeviceIdType.MESH)

    def res_first(d, u):
        return pltpu.make_async_remote_copy(
            src_ref=f_v.at[d, lax.rem(u, 2)], dst_ref=out.at[rows_of(u), pl.ds(first_col[d], half)],
            send_sem=res_sent.at[d, u], recv_sem=res_got.at[d, u],
            device_id={'tp': behind[d]}, device_id_type=pl.DeviceIdType.MESH)

    def res_pass(d, u):
        here = out.at[rows_of(u), pl.ds(first_col[d], half)]
        return pltpu.make_async_remote_copy(
            src_ref=here, dst_ref=here, send_sem=res_sent.at[d, u], recv_sem=res_got.at[d, u],
            device_id={'tp': behind[d]}, device_id_type=pl.DeviceIdType.MESH)

    def inside(u):
        return (u >= 0) & (u < chunks)

    def step(index, carry):
        t = index - 2
        chunk = [t - LAG * place[d] for d in range(2)]
        for d in range(2):
            u = chunk[d]

            @pl.when(inside(u) & (place[d] > 0))
            def _():
                sum_send(d, u).wait_recv()
                r_copy(d, u).start()

            @pl.when(inside(u) & (place[d] == last))
            def _():
                x_copy(d, u).start()

        for d in range(2):
            u = chunk[d]
            slot = lax.rem(u + 2, 2)

            @pl.when(inside(u) & (place[d] > 0))
            def _():
                r_copy(d, u).wait()

            @pl.when(inside(u) & (place[d] > 0) & (place[d] < last))
            def _():
                p_v[d, slot] = p_v[d, slot] + r_v[d]

            @pl.when(inside(u) & (place[d] < last))
            def _():
                sum_send(d, u).start()

            @pl.when(inside(u) & (place[d] == last))
            def _():
                x_copy(d, u).wait()
                f_v[d, slot] = (x_v[d].astype(jnp.float32) + (p_v[d, slot] + r_v[d])).astype(jnp.bfloat16)
                f_copy(d, u).start()
                res_first(d, u).start()

        for d in range(2):
            v = t - LAG * last - LAG_BACK * (last - place[d])

            @pl.when(inside(v) & (place[d] > 0) & (place[d] < last))
            def _():
                res_pass(d, v).wait_recv()
                res_pass(d, v).start()

        for d in range(2):
            u = chunk[d]

            @pl.when(inside(u + 2))
            def _():
                a_copy(d, u + 2).start()

            @pl.when(inside(u + 1))
            def _():
                slot = lax.rem(u + 1, 2)

                @pl.when(inside(u - 1) & (place[d] < last))
                def _():
                    sum_send(d, u - 1).wait_send()

                @pl.when(inside(u - 1) & (place[d] == last))
                def _():
                    f_copy(d, u - 1).wait()
                    res_first(d, u - 1).wait_send()

                a_copy(d, u + 1).wait()

                def column_tile(j, carry):
                    cols = pl.ds(pl.multiple_of(j * tile, tile), tile)
                    w_cols = pl.ds(pl.multiple_of(first_col[d] + j * tile, tile), tile)

                    @pl.when(u == -1)
                    def _():
                        w_copy(first_col[d] // tile + j).wait()

                    p_v[d, slot, :, cols] = jnp.dot(a_v[d, slot], w_v[:, w_cols], preferred_element_type=jnp.float32)
                    return carry

                lax.fori_loop(0, tiles // 2, column_tile, 0)
        return carry

    lax.fori_loop(0, chunks + 2 + LAG * last + LAG_BACK * (last - 1), step, 0)

    for d in range(2):
        for u in (chunks - 2, chunks - 1):
            @pl.when(place[d] < last)
            def _():
                sum_send(d, u).wait_send()

            @pl.when(place[d] == last)
            def _():
                f_copy(d, u).wait()
                res_first(d, u).wait_send()

        def drain(u, carry):
            @pl.when((place[d] > 0) & (place[d] < last))
            def _():
                res_pass(d, u).wait_send()

            @pl.when(place[d] == 0)
            def _():
                res_pass(d, u).wait_recv()
            return carry

        lax.fori_loop(0, chunks, drain, 0)


def chain_sum(attn, w_o, x_rows, n_tp, size):
    rows, inner = attn.shape
    width = w_o.shape[1]
    half = width // 2
    chunks = rows // size
    tiles = 2 * max(1, half // 512)
    sems = pltpu.SemaphoreType.DMA
    out, _, _ = pl.pallas_call(
        functools.partial(chain_kernel, n_tp, size),
        out_shape=(jax.ShapeDtypeStruct((rows, width), jnp.bfloat16),
                   jax.ShapeDtypeStruct((rows, half), jnp.float32),
                   jax.ShapeDtypeStruct((rows, half), jnp.float32)),
        in_specs=[pl.BlockSpec(memory_space=pl.ANY)] * 3,
        out_specs=(pl.BlockSpec(memory_space=pl.ANY),) * 3,
        scratch_shapes=[
            pltpu.VMEM((inner, width), jnp.bfloat16),
            pltpu.VMEM((2, 2, size, inner), jnp.bfloat16),
            pltpu.VMEM((2, 2, size, half), jnp.float32),
            pltpu.VMEM((2, size, half), jnp.float32),
            pltpu.VMEM((2, size, half), jnp.bfloat16),
            pltpu.VMEM((2, 2, size, half), jnp.bfloat16),
            sems((tiles,)), sems((2, 2)), sems((2,)), sems((2,)), sems((2, 2)),
            sems((2, chunks)), sems((2, chunks)), sems((2, chunks)), sems((2, chunks)),
        ],
        compiler_params=pltpu.CompilerParams(collective_id=0, has_side_effects=True,
                                             vmem_limit_bytes=60 * 1024 * 1024),
        cost_estimate=pl.CostEstimate(flops=2 * rows * inner * width, transcendentals=0,
                                      bytes_accessed=2 * inner * width + 12 * rows * width),
        name="chain_sum",
    )(attn, w_o, x_rows)
    return out


def solution(mesh):
    n_tp = mesh.shape['tp']
    n_cp = mesh.shape['cp']

    def local_step(x_blk, pos_blk, w_dq, g_q, w_uq, w_dkv, g_kv, w_uk, w_uv, w_o):
        num_seq, seq_dev, width = x_blk.shape
        kv_rank = g_kv.shape[0]
        rope_dim = w_dkv.shape[1] - kv_rank
        heads_dev = (w_uq.shape[1] - w_uk.shape[1]) // rope_dim
        nope_dim = w_uk.shape[1] // heads_dev
        soft_scale = (nope_dim + rope_dim) ** -0.5
        n_blocks = 2 * n_cp
        block_len = seq_dev // 2
        n_pairs = heads_dev // PAIR
        pos_f32 = pos_blk.astype(jnp.float32)
        x_flat = x_blk.reshape(num_seq * seq_dev, width)

        cos_t, sin_t = rope_tables(pos_f32.reshape(-1), rope_dim)
        tables = (jnp.concatenate([cos_t, cos_t], axis=1), jnp.concatenate([-sin_t, sin_t], axis=1))
        kv_joint = jnp.dot(x_flat, w_dkv, preferred_element_type=jnp.float32).astype(jnp.bfloat16)
        latent = rms_norm(kv_joint[:, :kv_rank], g_kv)
        k_rope = rotate(kv_joint[:, kv_rank:], cos_t, sin_t)
        block_ids = jnp.floor(pos_f32.reshape(-1) / block_len)[:, None].astype(jnp.bfloat16)
        both = jnp.concatenate([latent, k_rope, jnp.broadcast_to(block_ids, k_rope.shape)], axis=1)
        both = both.reshape(num_seq, seq_dev, -1)

        def gather(lo, hi):
            everyone = lax.all_gather(both[lo:hi], 'cp', axis=1, tiled=True).reshape(hi - lo, n_blocks, block_len, -1)
            ids_all = everyone[:, :, 0, kv_rank + rope_dim].astype(jnp.int32)
            blocks = jnp.arange(n_blocks, dtype=jnp.int32)
            where = jnp.sum(jnp.where(ids_all[:, None, :] == blocks[:, None], blocks, 0), axis=2)
            order = jnp.concatenate([where, pos_blk[lo:hi, :1] // block_len], axis=1).astype(jnp.int32)
            return everyone, order

        def q_of(rows):
            q_latent = jnp.dot(rows, w_dq, preferred_element_type=jnp.float32).astype(jnp.bfloat16)
            return jnp.dot(rms_norm(q_latent, g_q), w_uq, preferred_element_type=jnp.float32).astype(jnp.bfloat16)

        everyone, order = gather(0, 1)
        everyone_r, order_r = gather(1, num_seq)
        attn = attend(q_of(x_flat[:seq_dev]), *tables, everyone, order[0], w_uk, w_uv, heads_dev, soft_scale, 0, 0,
                      range(n_pairs), None)
        share = jnp.dot(attn, w_o, preferred_element_type=jnp.float32)
        x_flat, share = together(x_flat, share)
        mine = lax.psum_scatter(share, 'tp', scatter_dimension=0, tiled=True)
        q_rest = q_of(x_flat[seq_dev:])
        attn = None
        for n in range(num_seq - 1):
            attn = attend(q_rest, *tables, everyone_r, order_r[n], w_uk, w_uv, heads_dev, soft_scale, n, n + 1,
                          range(n_pairs), attn)
        attn, mine = together(attn, mine)
        own = mine.shape[0]
        x_own = lax.dynamic_slice(x_flat, (lax.axis_index('tp') * own, 0), (own, width))
        first_own = (x_own.astype(jnp.float32) + mine).astype(jnp.bfloat16)
        out_first = lax.all_gather(first_own, 'tp', axis=0, tiled=True)
        out_rest = chain_sum(attn, w_o, x_flat, n_tp, CHUNK)
        out = jnp.concatenate([out_first, out_rest], axis=0).reshape(x_blk.shape)
        return out, latent.reshape(num_seq, seq_dev, -1), k_rope.reshape(num_seq, seq_dev, -1)

    seq_spec = P('dp', 'cp', None)
    in_specs = (seq_spec, P('dp', 'cp'), P(None, None), P(None), P(None, 'tp'), P(None, None), P(None),
                P(None, 'tp'), P(None, 'tp'), P('tp', None))
    return jax.shard_map(local_step, mesh=mesh, in_specs=in_specs,
                         out_specs=(seq_spec, seq_spec, seq_spec), check_vma=False)
```

```python
import functools

import jax
import jax.numpy as jnp
from jax import lax
from jax.experimental import pallas as pl
from jax.experimental.pallas import tpu as pltpu
from jax.sharding import PartitionSpec as P

ROPE_BASE = 10000.0
NORM_EPS = 1e-6
LOG2_E = 1.4426950408889634
CHUNK = 16
LAG = 2
LAG_BACK = 2
PAIR = 2


def rms_norm(tensor, norm_gain):
    tensor_f32 = tensor.astype(jnp.float32)
    inv_rms = lax.rsqrt(jnp.mean(tensor_f32 * tensor_f32, axis=-1, keepdims=True) + NORM_EPS)
    return (tensor_f32 * inv_rms * norm_gain).astype(jnp.bfloat16)


def rope_tables(positions, rope_dim):
    inv_freq = ROPE_BASE ** (-2.0 * jnp.arange(rope_dim // 2, dtype=jnp.float32) / rope_dim)
    angles = positions.astype(jnp.float32)[..., None] * inv_freq
    return jnp.cos(angles), jnp.sin(angles)


def rotate(tensor, cos_t, sin_t):
    tensor_f32 = tensor.astype(jnp.float32)
    half_dim = tensor_f32.shape[-1] // 2
    lower_half = tensor_f32[..., :half_dim]
    upper_half = tensor_f32[..., half_dim:]
    return jnp.concatenate([lower_half * cos_t - upper_half * sin_t,
                            lower_half * sin_t + upper_half * cos_t], axis=-1).astype(jnp.bfloat16)


def attend_kernel(soft_scale, row, order_ref, q_ref, cos_ref, sin_ref, lat_hbm, w_uk_ref, w_uv_ref, *rest):
    o_ref, lat_s, sems = rest[-3:]
    n_blocks, block_len = lat_hbm.shape[1:3]
    half_keys = n_blocks // 2 * block_len
    rank = w_uk_ref.shape[0]
    rope_dim = cos_ref.shape[1]
    nope_dim = w_uk_ref.shape[1] // PAIR
    v_dim = w_uv_ref.shape[1] // PAIR
    qk_dim = nope_dim + rope_dim

    @pl.when(pl.program_id(0) == 0)
    def _():
        copies = [pltpu.make_async_copy(lat_hbm.at[row, order_ref[j]], lat_s.at[pl.ds(j * block_len, block_len)],
                                        sems.at[j])
                  for j in range(n_blocks)]
        for copy in copies:
            copy.start()
        for copy in copies:
            copy.wait()

    low_id = order_ref[n_blocks]
    latent = lat_s[:, :rank]
    k_rope = lat_s[:, rank:rank + rope_dim]
    k_pair = jnp.dot(latent, w_uk_ref[...], preferred_element_type=jnp.float32).astype(jnp.bfloat16)

    q_pair = q_ref[...].astype(jnp.float32)
    cos2 = cos_ref[...]
    sin2 = sin_ref[...]
    col_minus_row = (lax.broadcasted_iota(jnp.int32, (block_len, half_keys), 1)
                     - lax.broadcasted_iota(jnp.int32, (block_len, half_keys), 0))
    low_mask = col_minus_row <= low_id * block_len
    high_mask = col_minus_row <= (n_blocks - 1 - low_id) * block_len - half_keys
    factor = soft_scale * LOG2_E
    contract_last = (((1,), (1,)), ((), ()))

    def scores(head):
        q_head = q_pair if head == 0 else pltpu.roll(q_pair, (PAIR - head) * qk_dim, 1)
        q_rope = q_head[:, nope_dim:qk_dim]
        swapped = jnp.concatenate([q_rope[:, rope_dim // 2:], q_rope[:, :rope_dim // 2]], axis=1)
        q_rot = q_rope * cos2 + swapped * sin2
        q_cat = jnp.concatenate([q_head[:, :nope_dim], q_rot], axis=1).astype(jnp.bfloat16)
        k_cat = jnp.concatenate([k_pair[:, head * nope_dim:(head + 1) * nope_dim], k_rope], axis=1)
        early = lax.dot_general(q_cat, k_cat[:half_keys], contract_last, preferred_element_type=jnp.float32)
        late = lax.dot_general(q_cat[block_len:], k_cat[half_keys:], contract_last,
                               preferred_element_type=jnp.float32)
        return early, late

    def low_probs(early):
        low = jnp.where(low_mask, early[:block_len], -jnp.inf)
        low_exp = jnp.exp2((low - jnp.max(low, axis=1, keepdims=True)) * factor)
        return (low_exp * (1.0 / jnp.sum(low_exp, axis=1, keepdims=True))).astype(jnp.bfloat16)

    def high_probs(early, late):
        near = early[block_len:]
        far = jnp.where(high_mask, late, -jnp.inf)
        top = jnp.maximum(jnp.max(near, axis=1, keepdims=True), jnp.max(far, axis=1, keepdims=True))
        near_exp = jnp.exp2((near - top) * factor)
        far_exp = jnp.exp2((far - top) * factor)
        inv_sum = 1.0 / (jnp.sum(near_exp, axis=1, keepdims=True) + jnp.sum(far_exp, axis=1, keepdims=True))
        return (near_exp * inv_sum).astype(jnp.bfloat16), (far_exp * inv_sum).astype(jnp.bfloat16)

    def low_value(head, probs):
        cols = slice(head * v_dim, (head + 1) * v_dim)
        o_ref[:block_len, cols] = jnp.dot(probs, v_pair[:half_keys, cols],
                                          preferred_element_type=jnp.float32).astype(jnp.bfloat16)

    def high_value(head, near, far):
        cols = slice(head * v_dim, (head + 1) * v_dim)
        o_ref[block_len:, cols] = (jnp.dot(near, v_pair[:half_keys, cols], preferred_element_type=jnp.float32)
                                   + jnp.dot(far, v_pair[half_keys:, cols],
                                             preferred_element_type=jnp.float32)).astype(jnp.bfloat16)

    first = scores(0)
    v_pair = jnp.dot(latent, w_uv_ref[...], preferred_element_type=jnp.float32).astype(jnp.bfloat16)
    low = low_probs(first[0])
    second = scores(1)
    high = high_probs(*first)
    low_value(0, low)
    low = low_probs(second[0])
    high_value(0, *high)
    high = high_probs(*second)
    low_value(1, low)
    high_value(1, *high)


def attend(q_full, cos2, sin2, lat_blocks, order, w_uk, w_uv, heads, soft_scale, row, prompt, pairs, prior):
    n_rows, n_blocks, block_len, width = lat_blocks.shape
    tokens = q_full.shape[0] // n_rows
    rank = w_uk.shape[0]
    keys = n_blocks * block_len
    qk_dim = q_full.shape[1] // heads
    nope_dim = w_uk.shape[1] // heads
    v_dim = w_uv.shape[1] // heads
    rope_dim = cos2.shape[1]
    first, count = pairs[0], len(pairs)
    flops = (2 * keys * rank * (nope_dim + v_dim) + 2 * tokens * keys * 3 // 4 * (qk_dim + v_dim)) * count * PAIR
    moved = 2 * (lat_blocks.size // n_rows + (tokens * (qk_dim + v_dim) + rank * (nope_dim + v_dim)) * count * PAIR)
    in_specs = [
        pl.BlockSpec((tokens, PAIR * qk_dim), lambda h, order: (row, h + first)),
        pl.BlockSpec((tokens, rope_dim), lambda h, order: (prompt, 0)),
        pl.BlockSpec((tokens, rope_dim), lambda h, order: (prompt, 0)),
        pl.BlockSpec(memory_space=pl.ANY),
        pl.BlockSpec((rank, PAIR * nope_dim), lambda h, order: (0, h + first)),
        pl.BlockSpec((rank, PAIR * v_dim), lambda h, order: (0, h + first)),
    ]
    operands = [q_full, cos2, sin2, lat_blocks, w_uk, w_uv]
    aliases = {}
    if prior is not None:
        in_specs.append(pl.BlockSpec(memory_space=pl.ANY))
        operands.append(prior)
        aliases = {len(operands): 0}
    return pl.pallas_call(
        functools.partial(attend_kernel, soft_scale, row),
        out_shape=jax.ShapeDtypeStruct((n_rows * tokens, heads * v_dim), jnp.bfloat16),
        grid_spec=pltpu.PrefetchScalarGridSpec(
            num_scalar_prefetch=1,
            grid=(count,),
            in_specs=in_specs,
            out_specs=pl.BlockSpec((tokens, PAIR * v_dim), lambda h, order: (row, h + first)),
            scratch_shapes=[pltpu.VMEM((keys, width), jnp.bfloat16), pltpu.SemaphoreType.DMA((n_blocks,))],
        ),
        input_output_aliases=aliases,
        compiler_params=pltpu.CompilerParams(dimension_semantics=("arbitrary",), vmem_limit_bytes=56 * 1024 * 1024),
        cost_estimate=pl.CostEstimate(flops=flops, bytes_accessed=moved,
                                      transcendentals=tokens * keys * count * PAIR * 3 // 4),
        name="attend",
    )(order, *operands)


def together(*values):
    return lax.optimization_barrier(values)


def chain_kernel(n_tp, size, attn, w_o, x_rows, out, got_up, got_dn, w_v, a_v, p_v, r_v, x_v, f_v,
                 w_sem, a_sem, r_sem, x_sem, f_sem, sum_sent, sum_got, res_sent, res_got):
    z = lax.axis_index('tp')
    last = n_tp - 1
    half = out.shape[1] // 2
    chunks = attn.shape[0] // size
    skip = x_rows.shape[0] - attn.shape[0]
    got = (got_up, got_dn)
    place = (z, last - z)
    ahead = (z + 1, z - 1)
    behind = (z - 1, z + 1)
    first_col = (half, 0)
    tile = w_v.shape[1] // w_sem.shape[0]

    barrier = pltpu.get_barrier_semaphore()
    for there, device in ((z > 0, z - 1), (z < last, z + 1)):
        @pl.when(there)
        def _():
            pl.semaphore_signal(barrier, inc=1, device_id={'tp': device}, device_id_type=pl.DeviceIdType.MESH)
    middle = (z > 0) & (z < last)

    @pl.when(middle)
    def _():
        pl.semaphore_wait(barrier, 2)

    @pl.when(jnp.logical_not(middle))
    def _():
        pl.semaphore_wait(barrier, 1)

    def w_copy(i):
        cols = pl.ds(i * tile if isinstance(i, int) else pl.multiple_of(i * tile, tile), tile)
        return pltpu.make_async_copy(w_o.at[:, cols], w_v.at[:, cols], w_sem.at[i])

    tiles = w_sem.shape[0]
    second = list(range(tiles // 2, tiles))
    first = list(range(tiles // 2))
    for near, wanted in ((z <= last // 2, second + first), (z > last // 2, first + second)):
        @pl.when(near)
        def _():
            for i in wanted:
                w_copy(i).start()

    def rows_of(u):
        return pl.ds(pl.multiple_of(u * size, size), size)

    def x_rows_of(u):
        return pl.ds(pl.multiple_of(skip + u * size, size), size)

    def a_copy(d, duo):
        slot = lax.rem(duo, 2)
        duo_rows = pl.ds(pl.multiple_of(duo * 2 * size, 2 * size), 2 * size)
        return pltpu.make_async_copy(attn.at[duo_rows], a_v.at[d, slot], a_sem.at[d, slot])

    def sum_at(d, u):
        return p_v.at[d, lax.rem(lax.div(u, 2), 2), lax.rem(u, 2)]

    def r_copy(d, u):
        return pltpu.make_async_copy(got[d].at[rows_of(u)], r_v.at[d], r_sem.at[d])

    def x_copy(d, u):
        return pltpu.make_async_copy(x_rows.at[x_rows_of(u), pl.ds(first_col[d], half)], x_v.at[d], x_sem.at[d])

    def f_copy(d, u):
        slot = lax.rem(u, 2)
        return pltpu.make_async_copy(f_v.at[d, slot], out.at[rows_of(u), pl.ds(first_col[d], half)],
                                     f_sem.at[d, slot])

    def sum_send(d, u):
        return pltpu.make_async_remote_copy(
            src_ref=sum_at(d, u), dst_ref=got[d].at[rows_of(u)],
            send_sem=sum_sent.at[d, u], recv_sem=sum_got.at[d, u],
            device_id={'tp': ahead[d]}, device_id_type=pl.DeviceIdType.MESH)

    def res_first(d, u):
        return pltpu.make_async_remote_copy(
            src_ref=f_v.at[d, lax.rem(u, 2)], dst_ref=out.at[rows_of(u), pl.ds(first_col[d], half)],
            send_sem=res_sent.at[d, u], recv_sem=res_got.at[d, u],
            device_id={'tp': behind[d]}, device_id_type=pl.DeviceIdType.MESH)

    def res_pass(d, u):
        here = out.at[rows_of(u), pl.ds(first_col[d], half)]
        return pltpu.make_async_remote_copy(
            src_ref=here, dst_ref=here, send_sem=res_sent.at[d, u], recv_sem=res_got.at[d, u],
            device_id={'tp': behind[d]}, device_id_type=pl.DeviceIdType.MESH)

    def inside(u):
        return (u >= 0) & (u < chunks)

    def step(index, carry):
        t = index - 2
        chunk = [t - LAG * place[d] for d in range(2)]
        for d in range(2):
            u = chunk[d]

            @pl.when(inside(u) & (place[d] > 0))
            def _():
                sum_send(d, u).wait_recv()
                r_copy(d, u).start()

            @pl.when(inside(u) & (place[d] == last))
            def _():
                x_copy(d, u).start()

        for d in range(2):
            u = chunk[d]
            slot = lax.rem(jnp.maximum(u, 0), 2)
            total = sum_at(d, jnp.maximum(u, 0))

            @pl.when(inside(u) & (place[d] > 0))
            def _():
                r_copy(d, u).wait()

            @pl.when(inside(u) & (place[d] > 0) & (place[d] < last))
            def _():
                total[...] = total[...] + r_v[d]

            @pl.when(inside(u) & (place[d] < last))
            def _():
                sum_send(d, u).start()

            @pl.when(inside(u) & (place[d] == last))
            def _():
                x_copy(d, u).wait()
                f_v[d, slot] = (x_v[d].astype(jnp.float32) + (total[...] + r_v[d])).astype(jnp.bfloat16)
                f_copy(d, u).start()
                res_first(d, u).start()

        for d in range(2):
            v = t - LAG * last - LAG_BACK * (last - place[d])

            @pl.when(inside(v) & (place[d] > 0) & (place[d] < last))
            def _():
                res_pass(d, v).wait_recv()
                res_pass(d, v).start()

        for d in range(2):
            u = chunk[d]

            @pl.when(inside(u + 1) & inside(u - 1) & (place[d] == last))
            def _():
                f_copy(d, u - 1).wait()
                res_first(d, u - 1).wait_send()

            @pl.when(inside(u + 2) & (lax.rem(t + 4, 2) == 0))
            def _():
                a_copy(d, lax.div(u + 2, 2)).start()

            @pl.when(inside(u + 1) & (lax.rem(t + 4, 2) == 1))
            def _():
                duo = lax.div(u + 1, 2)
                slot = lax.rem(duo, 2)

                @pl.when(inside(u - 3) & (place[d] < last))
                def _():
                    sum_send(d, u - 3).wait_send()
                    sum_send(d, u - 2).wait_send()

                a_copy(d, duo).wait()

                def column_tile(j, carry):
                    cols = pl.ds(pl.multiple_of(j * tile, tile), tile)
                    w_cols = pl.ds(pl.multiple_of(first_col[d] + j * tile, tile), tile)

                    @pl.when(u == -1)
                    def _():
                        w_copy(first_col[d] // tile + j).wait()

                    both = jnp.dot(a_v[d, slot], w_v[:, w_cols], preferred_element_type=jnp.float32)
                    p_v[d, slot, 0, :, cols] = both[:size]
                    p_v[d, slot, 1, :, cols] = both[size:]
                    return carry

                lax.fori_loop(0, tiles // 2, column_tile, 0)
        return carry

    lax.fori_loop(0, chunks + 2 + LAG * last + LAG_BACK * (last - 1), step, 0)

    for d in range(2):
        for u in range(chunks - 4, chunks):
            @pl.when(place[d] < last)
            def _():
                sum_send(d, u).wait_send()

        for u in (chunks - 2, chunks - 1):
            @pl.when(place[d] == last)
            def _():
                f_copy(d, u).wait()
                res_first(d, u).wait_send()

        def drain(u, carry):
            @pl.when((place[d] > 0) & (place[d] < last))
            def _():
                res_pass(d, u).wait_send()

            @pl.when(place[d] == 0)
            def _():
                res_pass(d, u).wait_recv()
            return carry

        lax.fori_loop(0, chunks, drain, 0)


def chain_sum(attn, w_o, x_rows, n_tp, size):
    rows, inner = attn.shape
    width = w_o.shape[1]
    half = width // 2
    chunks = rows // size
    tiles = 2 * max(1, half // 512)
    sems = pltpu.SemaphoreType.DMA
    out, _, _ = pl.pallas_call(
        functools.partial(chain_kernel, n_tp, size),
        out_shape=(jax.ShapeDtypeStruct((rows, width), jnp.bfloat16),
                   jax.ShapeDtypeStruct((rows, half), jnp.float32),
                   jax.ShapeDtypeStruct((rows, half), jnp.float32)),
        in_specs=[pl.BlockSpec(memory_space=pl.ANY)] * 3,
        out_specs=(pl.BlockSpec(memory_space=pl.ANY),) * 3,
        scratch_shapes=[
            pltpu.VMEM((inner, width), jnp.bfloat16),
            pltpu.VMEM((2, 2, 2 * size, inner), jnp.bfloat16),
            pltpu.VMEM((2, 2, 2, size, half), jnp.float32),
            pltpu.VMEM((2, size, half), jnp.float32),
            pltpu.VMEM((2, size, half), jnp.bfloat16),
            pltpu.VMEM((2, 2, size, half), jnp.bfloat16),
            sems((tiles,)), sems((2, 2)), sems((2,)), sems((2,)), sems((2, 2)),
            sems((2, chunks)), sems((2, chunks)), sems((2, chunks)), sems((2, chunks)),
        ],
        compiler_params=pltpu.CompilerParams(collective_id=0, has_side_effects=True,
                                             vmem_limit_bytes=60 * 1024 * 1024),
        cost_estimate=pl.CostEstimate(flops=2 * rows * inner * width, transcendentals=0,
                                      bytes_accessed=2 * inner * width + 12 * rows * width),
        name="chain_sum",
    )(attn, w_o, x_rows)
    return out


def solution(mesh):
    n_tp = mesh.shape['tp']
    n_cp = mesh.shape['cp']

    def local_step(x_blk, pos_blk, w_dq, g_q, w_uq, w_dkv, g_kv, w_uk, w_uv, w_o):
        num_seq, seq_dev, width = x_blk.shape
        kv_rank = g_kv.shape[0]
        rope_dim = w_dkv.shape[1] - kv_rank
        heads_dev = (w_uq.shape[1] - w_uk.shape[1]) // rope_dim
        nope_dim = w_uk.shape[1] // heads_dev
        soft_scale = (nope_dim + rope_dim) ** -0.5
        n_blocks = 2 * n_cp
        block_len = seq_dev // 2
        n_pairs = heads_dev // PAIR
        pos_f32 = pos_blk.astype(jnp.float32)
        x_flat = x_blk.reshape(num_seq * seq_dev, width)

        cos_t, sin_t = rope_tables(pos_f32.reshape(-1), rope_dim)
        tables = (jnp.concatenate([cos_t, cos_t], axis=1), jnp.concatenate([-sin_t, sin_t], axis=1))
        kv_joint = jnp.dot(x_flat, w_dkv, preferred_element_type=jnp.float32).astype(jnp.bfloat16)
        latent = rms_norm(kv_joint[:, :kv_rank], g_kv)
        k_rope = rotate(kv_joint[:, kv_rank:], cos_t, sin_t)
        block_ids = jnp.floor(pos_f32.reshape(-1) / block_len)[:, None].astype(jnp.bfloat16)
        both = jnp.concatenate([latent, k_rope, jnp.broadcast_to(block_ids, k_rope.shape)], axis=1)
        both = both.reshape(num_seq, seq_dev, -1)

        def gather(lo, hi):
            everyone = lax.all_gather(both[lo:hi], 'cp', axis=1, tiled=True).reshape(hi - lo, n_blocks, block_len, -1)
            ids_all = everyone[:, :, 0, kv_rank + rope_dim].astype(jnp.int32)
            blocks = jnp.arange(n_blocks, dtype=jnp.int32)
            where = jnp.sum(jnp.where(ids_all[:, None, :] == blocks[:, None], blocks, 0), axis=2)
            order = jnp.concatenate([where, pos_blk[lo:hi, :1] // block_len], axis=1).astype(jnp.int32)
            return everyone, order

        def q_of(rows):
            q_latent = jnp.dot(rows, w_dq, preferred_element_type=jnp.float32).astype(jnp.bfloat16)
            return jnp.dot(rms_norm(q_latent, g_q), w_uq, preferred_element_type=jnp.float32).astype(jnp.bfloat16)

        everyone, order = gather(0, 1)
        everyone_r, order_r = gather(1, num_seq)
        attn = attend(q_of(x_flat[:seq_dev]), *tables, everyone, order[0], w_uk, w_uv, heads_dev, soft_scale, 0, 0,
                      range(n_pairs), None)
        share = jnp.dot(attn, w_o, preferred_element_type=jnp.float32)
        x_flat, share = together(x_flat, share)
        mine = lax.psum_scatter(share, 'tp', scatter_dimension=0, tiled=True)
        q_rest = q_of(x_flat[seq_dev:])
        attn = None
        for n in range(num_seq - 1):
            attn = attend(q_rest, *tables, everyone_r, order_r[n], w_uk, w_uv, heads_dev, soft_scale, n, n + 1,
                          range(n_pairs), attn)
        attn, mine = together(attn, mine)
        own = mine.shape[0]
        x_own = lax.dynamic_slice(x_flat, (lax.axis_index('tp') * own, 0), (own, width))
        first_own = (x_own.astype(jnp.float32) + mine).astype(jnp.bfloat16)
        out_first = lax.all_gather(first_own, 'tp', axis=0, tiled=True)
        out_rest = chain_sum(attn, w_o, x_flat, n_tp, CHUNK)
        out = jnp.concatenate([out_first, out_rest], axis=0).reshape(x_blk.shape)
        return out, latent.reshape(num_seq, seq_dev, -1), k_rope.reshape(num_seq, seq_dev, -1)

    seq_spec = P('dp', 'cp', None)
    in_specs = (seq_spec, P('dp', 'cp'), P(None, None), P(None), P(None, 'tp'), P(None, None), P(None),
                P(None, 'tp'), P(None, 'tp'), P('tp', None))
    return jax.shard_map(local_step, mesh=mesh, in_specs=in_specs,
                         out_specs=(seq_spec, seq_spec, seq_spec), check_vma=False)
```
